32 devices in a mesh: gx: 2 (over x), gy: 4 (over y, core), gz: 4 (over z).
Axes of the slice: x: 2, y: 2, z: 4, core: 2. Of those that a mesh axis runs over, the one named last changes fastest.
Arguments:
- inputs: bfloat16 [640, 8192], P(('gx', 'gz'), 'gy'), may hold values from -6 to 6
- out_grad: bfloat16 [640, 8192], P(('gx', 'gz'), 'gy'), may hold values from -6 to 6
- gate_weight: bfloat16 [8192, 16384], P('gy', ('gx', 'gz')), may hold values from -0.0625 to 0.0625
- up_weight: bfloat16 [8192, 16384], P('gy', ('gx', 'gz')), may hold values from -0.0625 to 0.0625
- down_weight: bfloat16 [16384, 8192], P(('gx', 'gz'), 'gy'), may hold values from -0.046875 to 0.046875
Outputs:
- in_grad: bfloat16 [640, 8192], P(('gx', 'gz'), 'gy')
The draws below stay inside these ranges and needn't reach their ends.
All inputs are finite; a program needn't handle non-finite values.
Results may differ from the reference program's by a relative error of at most 0.0049.
Values may be sent and summed in bfloat16 or wider, within the bound.
A program may use at most 128 MiB of HBM per device.

```python
import jax
import jax.numpy as jnp
from jax import lax

D = 8192
FF = 16384
TOKENS = 640


def shard_levels(rng, shape, split, least, top_value):
    gain = 1.0
    for dim, shards_of in split:
        heights = jax.random.uniform(jax.random.fold_in(jax.random.fold_in(rng, 6), dim), (shards_of,), jnp.float32, least / len(split), top_value / len(split))
        gain = gain * jnp.repeat(jnp.exp(heights), shape[dim] // shards_of).reshape((-1,) + (1,) * (len(shape) - 1 - dim))
    return gain


def bell_draw(key, shape, deviation, bound, pieces=(), held_as=jnp.bfloat16):
    factor_of = shard_levels(key, shape, pieces, -0.22, 0.18) if pieces else 1.0
    result = jax.random.normal(key, shape, jnp.float32) * deviation * factor_of
    return jnp.minimum(jnp.maximum(result, -bound), bound).astype(held_as)


def setup_inputs(seed: int = 0) -> dict:
    arg_keys = jax.random.split(jax.random.key(seed), 6)
    return {
        "inputs": bell_draw(arg_keys[0], (TOKENS, D), 1.0, 6.0, ((0, 8), (1, 4))),
        "out_grad": bell_draw(arg_keys[1], (TOKENS, D), 1.0, 6.0, ((0, 8), (1, 4))),
        "gate_weight": bell_draw(arg_keys[2], (D, FF), D ** -0.5, 0.0625, ((0, 4), (1, 8))),
        "up_weight": bell_draw(arg_keys[3], (D, FF), D ** -0.5, 0.0625, ((0, 4), (1, 8))),
        "down_weight": bell_draw(arg_keys[4], (FF, D), FF ** -0.5, 0.046875, ((0, 8), (1, 4))),
    }


def contract_last(left, right):
    return lax.dot_general(left, right, (((1,), (1,)), ((), ())), preferred_element_type=jnp.float32)


def reference(inputs, out_grad, gate_weight, up_weight, down_weight):
    gate = jnp.dot(inputs, gate_weight, preferred_element_type=jnp.float32)
    upper = jnp.dot(inputs, up_weight, preferred_element_type=jnp.float32)
    hidden_grad = contract_last(out_grad, down_weight)
    logistic = jax.nn.sigmoid(gate)
    gate_grad = (hidden_grad * upper * logistic * (1.0 + gate * (1.0 - logistic))).astype(jnp.bfloat16)
    up_grad = (hidden_grad * gate * logistic).astype(jnp.bfloat16)
    total = contract_last(gate_grad, gate_weight) + contract_last(up_grad, up_weight)
    return total.astype(jnp.bfloat16)
```

```python
import functools

import jax
import jax.numpy as jnp
from jax import lax
from jax.experimental import pallas as pl
from jax.experimental.pallas import tpu as pltpu
from jax.sharding import PartitionSpec as P

F32, BF16 = jnp.float32, jnp.bfloat16
MESH = pl.DeviceIdType.MESH
SPECS = (
    P(("gx", "gz"), "gy"),
    P(("gx", "gz"), "gy"),
    P("gy", ("gx", "gz")),
    P("gy", ("gx", "gz")),
    P(("gx", "gz"), "gy"),
)
OUT_SPEC = P(("gx", "gz"), "gy")


def contract_last(left, right):
    return lax.dot_general(left, right, (((1,), (1,)), ((), ())), preferred_element_type=F32)


def grads_of(gate, upper, hidden_grad):
    logistic = jax.nn.sigmoid(gate)
    gate_grad = hidden_grad * upper * logistic * (1.0 + gate * (1.0 - logistic))
    up_grad = hidden_grad * gate * logistic
    return gate_grad.astype(BF16), up_grad.astype(BF16)


ORDER = {0: (1, 2, 3), 1: (0, 2, 3), 2: (3, 1, 0), 3: (2, 1, 0)}
CHUNKS = 5
QUARTERS = 4
PIECES = 4


def kernel(
    rows, depth, width,
    x_hbm, og_hbm, gw_hbm, uw_hbm, dw_hbm, out_ref,
    xbuf, gw, uw, dw, pbuf, drecv, mine, ysend, yrecv, gbuf, xs, xr, wb, zs, zr,
    in_sem, w_sem, ag_recv, agx_send, agz_send, d_send, d_recv, y_send, y_recv,
    gy_send, gy_recv, gd_send, gd_recv, x_send, x_recv, z_send, z_recv,
):
    gx, gy, gz = lax.axis_index("gx"), lax.axis_index("gy"), lax.axis_index("gz")
    where_y, core = gy // 2, gy % 2
    mate = gy + 1 - 2 * core
    over = gy + 2 - 4 * where_y
    across = 1 - gx
    both = 2 * rows
    quarter = width // QUARTERS
    piece = depth // PIECES

    def remote(src, dst, send, recv, **where):
        return pltpu.make_async_remote_copy(
            src_ref=src, dst_ref=dst, send_sem=send, recv_sem=recv,
            device_id=where, device_id_type=MESH,
        )

    def slot(j):
        return pl.ds(pl.multiple_of(j * rows, 16), rows)

    def columns(q):
        return pl.ds(pl.multiple_of(q * quarter, 128), quarter)

    def gather_x(k):
        return remote(
            xbuf.at[:, slot(2 * k + 1), :], xbuf.at[:, slot(2 * k + 2), :],
            agx_send.at[k], ag_recv.at[2 * k + 2], gx=across,
        )

    def gather_z(src, dst, way, n, to):
        return remote(
            xbuf.at[:, slot(src), :], xbuf.at[:, slot(dst), :],
            agz_send.at[way, n], ag_recv.at[dst], gz=to,
        )

    def mate_sums(s, t):
        return remote(
            pbuf.at[t], drecv.at[s % 2, t], d_send.at[t], d_recv.at[s % 2, t], gy=mate
        )

    def over_sums(s, h):
        part = pl.ds(h * rows, rows)
        return remote(
            ysend.at[s, :, part, :], yrecv.at[s, :, part, :],
            y_send.at[s, h], y_recv.at[s, h], gy=over,
        )

    def over_grads(s, h, q):
        block = gbuf.at[:, slot(2 * s + h), columns(q)]
        return remote(block, block, gy_send.at[s, h], gy_recv.at[s, h], gy=over)

    def mate_grads(s, q, n):
        chunk = pl.ds(pl.multiple_of(s * both, 16), both)
        block = gbuf.at[:, chunk, columns(q)]
        return remote(block, block, gd_send.at[s, n], gd_recv.at[s, n], gy=mate)

    def out_x(s, n):
        return remote(xs.at[s, n], xr.at[s, n], x_send.at[s, n], x_recv.at[s, n], gx=across)

    def out_z(k, n, to):
        return remote(zs.at[k, n], zr.at[gz, n], z_send.at[k, n], z_recv.at[gz, n], gz=to)

    def in_z(src, n):
        return remote(zs.at[0, n], zr.at[src, n], z_send.at[0, n], z_recv.at[src, n], gz=src)

    def place_of(k):
        place = ORDER[0][k - 1]
        for z in range(1, 4):
            place = jnp.where(gz == z, ORDER[z][k - 1], place)
        return place

    def quarter_of(t):
        y_of = where_y + (1 - t % 2) * (1 - 2 * where_y)
        core_of = core + (1 - t // 2) * (1 - 2 * core)
        return 2 * y_of + core_of

    def load_weights(t):
        q = quarter_of(t)
        return [
            pltpu.make_async_copy(gw_hbm.at[:, columns(q)], gw.at[:, columns(q)], w_sem.at[0, t]),
            pltpu.make_async_copy(uw_hbm.at[:, columns(q)], uw.at[:, columns(q)], w_sem.at[1, t]),
            pltpu.make_async_copy(dw_hbm.at[columns(q), :], dw.at[columns(q), :], w_sem.at[2, t]),
        ]

    load_in = [
        pltpu.make_async_copy(ref, xbuf.at[i, slot(1), :], in_sem.at[i])
        for i, ref in enumerate((x_hbm, og_hbm))
    ]
    for copy in load_in:
        copy.start()
    for t in range(QUARTERS):
        for copy in load_weights(t):
            copy.start()

    barrier = pltpu.get_barrier_semaphore()
    pl.semaphore_signal(barrier, inc=1, device_id={"gy": mate}, device_id_type=MESH)
    pl.semaphore_signal(barrier, inc=1, device_id={"gy": over}, device_id_type=MESH)
    pl.semaphore_signal(barrier, inc=1, device_id={"gx": across}, device_id_type=MESH)
    for step in range(1, 4):
        pl.semaphore_signal(
            barrier, inc=1, device_id={"gz": (gz + step) % 4}, device_id_type=MESH
        )
    pl.semaphore_wait(barrier, 6)
    for copy in load_in:
        copy.wait()

    def landing(to, src):
        return 2 * ORDER[to].index(src) + 3

    def z_sends(z, first):
        copies = []
        for way, step in ((0, 1), (1, -1)):
            if not 0 <= z + step < 4:
                continue
            n = 0
            src = z
            while 0 <= src < 4:
                from_slot = 1 if src == z else landing(z, src)
                wave = abs(src - z)
                if wave in first:
                    copies.append(gather_z(from_slot, landing(z + step, src), way, n, z + step))
                n += 1
                src -= step
        return copies

    def at_place(z):
        return pl.when(gz == z)

    gather_x(0).start()
    for z in range(4):
        @at_place(z)
        def _(z=z):
            for copy in z_sends(z, (0,)):
                copy.start()

    def arrive(k):
        slot_k = 2 * k + 1
        gather_z(1, slot_k, 0, 0, 0 * gz).wait_recv()

    def forward_step(s):
        for z in range(4):
            @at_place(z)
            def _(z=z):
                middle = z in (1, 2)
                waits = {1: (1, 2), 2: (3,), 3: ()}[s] if middle else (s,)
                for k in waits:
                    arrive(k)
                for copy in z_sends(z, (s,)):
                    copy.start()
                for k in waits:
                    gather_x(k).start()

    def has_first(s):
        return s >= 1

    def has_second(s):
        return s <= CHUNKS - 2

    def each_half(s, act):
        pl.when(has_first(s))(lambda: act(0))
        pl.when(has_second(s))(lambda: act(1))

    def project(s):
        for step in range(1, 4):
            pl.when(s == step)(functools.partial(forward_step, step))

        @pl.when(s >= 1)
        def _():
            gather_x(s - 1).wait_recv()
            for t in range(2):
                mate_sums(s - 1, t).wait_send()

        chunk = pl.ds(pl.multiple_of(s * both, 16), both)

        def one(t, carry):
            q = quarter_of(t)

            @pl.when(s == 0)
            def _():
                for copy in load_weights(t):
                    copy.wait()

            x = xbuf[0, chunk, :]
            pbuf[t, 0] = jnp.dot(x, gw[:, columns(q)], preferred_element_type=F32)
            pbuf[t, 1] = jnp.dot(x, uw[:, columns(q)], preferred_element_type=F32)
            pbuf[t, 2] = contract_last(xbuf[1, chunk, :], dw[columns(q), :])

            @pl.when(t < 2)
            def _():
                mate_sums(s, t).start()

            @pl.when(t == 2)
            def _():
                mate_sums(s, 0).wait_recv()

                def add(r, carry):
                    part = pl.ds(pl.multiple_of(r * 16, 16), 16)
                    for i in range(3):
                        total = pbuf[2, i, part, :] + drecv[s % 2, 0, i, part, :]
                        ysend[s, i, part, :] = total.astype(BF16)
                    return carry

                lax.fori_loop(0, both // 16, add, 0)
                each_half(s, lambda h: over_sums(s, h).start())

            @pl.when(t == 3)
            def _():
                mate_sums(s, 1).wait_recv()

                def add(r, carry):
                    part = pl.ds(pl.multiple_of(r * 16, 16), 16)
                    for i in range(3):
                        mine[s % 2, i, part, :] = pbuf[3, i, part, :] + drecv[s % 2, 1, i, part, :]
                    return carry

                lax.fori_loop(0, both // 16, add, 0)

            return carry

        lax.fori_loop(0, QUARTERS, one, 0)

    def differentiate(s):
        each_half(s, lambda h: over_sums(s, h).wait_recv())

        def block(r, carry):
            part = pl.ds(pl.multiple_of(r * 16, 16), 16)
            terms = [mine[s % 2, i, part, :] + yrecv[s, i, part, :].astype(F32) for i in range(3)]
            here = pl.ds(pl.multiple_of(s * both + r * 16, 16), 16)
            gbuf[0, here, columns(gy)], gbuf[1, here, columns(gy)] = grads_of(*terms)
            return carry

        lax.fori_loop(0, both // 16, block, 0)
        each_half(s, lambda h: over_grads(s, h, gy).start())
        mate_grads(s, gy, 0).start()

    def backproject(s):
        each_half(s, lambda h: over_grads(s, h, over).wait_recv())
        mate_grads(s, over, 1).start()
        mate_grads(s, mate, 0).wait_recv()
        mate_grads(s, mate + over - gy, 1).wait_recv()
        chunk = pl.ds(pl.multiple_of(s * both, 16), both)

        def one(n, carry):
            here = pl.ds(pl.multiple_of(n * piece, 128), piece)
            part = contract_last(gbuf[0, chunk, :], gw[here, :])
            part = part + contract_last(gbuf[1, chunk, :], uw[here, :])

            @pl.when(has_first(s))
            def _():
                xs[s, n] = part[:rows].astype(BF16)

            @pl.when(has_second(s))
            def _():
                wb[s, n] = part[rows:]

            @pl.when(has_first(s))
            def _():
                out_x(s, n).start()

            return carry

        lax.fori_loop(0, PIECES, one, 0)

    def pass_on(k):
        to = place_of(1)
        for j in range(2, 4):
            to = jnp.where(k == j, place_of(j), to)

        def one(n, carry):
            out_x(k + 1, n).wait_recv()
            zs[k, n] = (wb[k, n] + xr[k + 1, n].astype(F32)).astype(BF16)
            out_z(k, n, to).start()
            return carry

        lax.fori_loop(0, PIECES, one, 0)

    def stage(s, carry):
        pl.when(s == 1)(lambda: differentiate(s - 1))
        pl.when(s < CHUNKS)(lambda: project(s))
        pl.when((s >= 2) & (s <= CHUNKS))(lambda: differentiate(s - 1))
        pl.when(s >= 5)(lambda: pass_on(s - 4))
        pl.when((s >= 2) & (s <= CHUNKS + 1))(lambda: backproject(s - 2))
        return carry

    lax.fori_loop(0, CHUNKS + 3, stage, 0)

    for n in range(PIECES):
        out_x(1, n).wait_recv()
        total = wb[0, n] + xr[1, n].astype(F32)
        for step in range(1, 4):
            src = (gz + step) % 4
            in_z(src, n).wait_recv()
            total = total + zr[src, n].astype(F32)
        out_ref[:, n * piece : (n + 1) * piece] = total.astype(BF16)

    for k in range(4):
        gather_x(k).wait_send()
    for z in range(4):
        @at_place(z)
        def _(z=z):
            for copy in z_sends(z, (0, 1, 2)):
                copy.wait_send()
    for t in range(2):
        mate_sums(CHUNKS - 1, t).wait_send()

    def drain(s, carry):
        def half(h):
            over_sums(s, h).wait_send()
            over_grads(s, h, gy).wait_send()

        each_half(s, half)
        mate_grads(s, gy, 0).wait_send()
        mate_grads(s, over, 1).wait_send()

        @pl.when(has_first(s))
        def _():
            for n in range(PIECES):
                out_x(s, n).wait_send()

        @pl.when((s >= 1) & (s <= 3))
        def _():
            for n in range(PIECES):
                out_z(s, n, (gz + 1) % 4).wait_send()

        return carry

    lax.fori_loop(0, CHUNKS, drain, 0)


def fused(inputs, out_grad, gate_weight, up_weight, down_weight):
    rows, depth = inputs.shape
    width = gate_weight.shape[1]
    both, quarter, piece = 2 * rows, width // QUARTERS, depth // PIECES
    dma = pltpu.SemaphoreType.DMA
    n = CHUNKS
    scratch = [
        pltpu.VMEM((2, n * both, depth), BF16),
        pltpu.VMEM((depth, width), BF16),
        pltpu.VMEM((depth, width), BF16),
        pltpu.VMEM((width, depth), BF16),
        pltpu.VMEM((4, 3, both, quarter), F32),
        pltpu.VMEM((2, 2, 3, both, quarter), F32),
        pltpu.VMEM((2, 3, both, quarter), F32),
        pltpu.VMEM((n, 3, both, quarter), BF16),
        pltpu.VMEM((n, 3, both, quarter), BF16),
        pltpu.VMEM((2, n * both, width), BF16),
        pltpu.VMEM((n, PIECES, rows, piece), BF16),
        pltpu.VMEM((n, PIECES, rows, piece), BF16),
        pltpu.VMEM((4, PIECES, rows, piece), F32),
        pltpu.VMEM((4, PIECES, rows, piece), BF16),
        pltpu.VMEM((4, PIECES, rows, piece), BF16),
        dma((2,)), dma((3, 4)), dma((2 * n,)), dma((4,)), dma((2, 4)), dma((2,)), dma((2, 2)),
        dma((n, 2)), dma((n, 2)), dma((n, 2)), dma((n, 2)), dma((n, 2)), dma((n, 2)),
        dma((n, PIECES)), dma((n, PIECES)), dma((4, PIECES)), dma((4, PIECES)),
    ]
    return pl.pallas_call(
        functools.partial(kernel, rows, depth, width),
        out_shape=jax.ShapeDtypeStruct((rows, depth), BF16),
        in_specs=[pl.BlockSpec(memory_space=pl.ANY)] * 5,
        out_specs=pl.BlockSpec(memory_space=pltpu.VMEM),
        scratch_shapes=scratch,
        compiler_params=pltpu.CompilerParams(
            collective_id=0, has_side_effects=True, vmem_limit_bytes=66 * 1024 * 1000
        ),
    )(inputs, out_grad, gate_weight, up_weight, down_weight)


def plain(nx, ny, nz):
    def layer(inputs, out_grad, gate_weight, up_weight, down_weight):
        both = lax.all_gather(jnp.stack([inputs, out_grad]), ("gx", "gz"), axis=1, tiled=True)
        gate = jnp.dot(both[0], gate_weight, preferred_element_type=F32)
        upper = jnp.dot(both[0], up_weight, preferred_element_type=F32)
        hidden = contract_last(both[1], down_weight)
        terms = lax.psum_scatter(
            jnp.stack([gate, upper, hidden]), "gy", scatter_dimension=1, tiled=True
        )
        grads = jnp.stack(grads_of(terms[0], terms[1], terms[2]))
        grads = lax.all_gather(grads, "gy", axis=1, tiled=True)
        total = contract_last(grads[0], gate_weight) + contract_last(grads[1], up_weight)
        total = lax.psum_scatter(total, ("gx", "gz"), scatter_dimension=0, tiled=True)
        return total.astype(BF16)

    return layer


def solution(mesh):
    nx, ny, nz = mesh.shape["gx"], mesh.shape["gy"], mesh.shape["gz"]
    body = fused if (nx, ny, nz) == (2, 4, 4) else plain(nx, ny, nz)
    return jax.shard_map(body, mesh=mesh, in_specs=SPECS, out_specs=OUT_SPEC, check_vma=False)
```

```python
import functools

import jax
import jax.numpy as jnp
from jax import lax
from jax.experimental import pallas as pl
from jax.experimental.pallas import tpu as pltpu
from jax.sharding import PartitionSpec as P

F32, BF16 = jnp.float32, jnp.bfloat16
MESH = pl.DeviceIdType.MESH
SPECS = (
    P(("gx", "gz"), "gy"),
    P(("gx", "gz"), "gy"),
    P("gy", ("gx", "gz")),
    P("gy", ("gx", "gz")),
    P(("gx", "gz"), "gy"),
)
OUT_SPEC = P(("gx", "gz"), "gy")


def contract_last(left, right):
    return lax.dot_general(left, right, (((1,), (1,)), ((), ())), preferred_element_type=F32)


def grads_of(gate, upper, hidden_grad):
    logistic = jax.nn.sigmoid(gate)
    gate_grad = hidden_grad * upper * logistic * (1.0 + gate * (1.0 - logistic))
    up_grad = hidden_grad * gate * logistic
    return gate_grad.astype(BF16), up_grad.astype(BF16)


ORDER = {0: (1, 2, 3), 1: (0, 2, 3), 2: (3, 1, 0), 3: (2, 1, 0)}
CHUNKS = 5
QUARTERS = 4
PIECES = 4


def kernel(
    rows, depth, width,
    x_hbm, og_hbm, gw_hbm, uw_hbm, dw_hbm, out_ref,
    xbuf, gw, uw, dw, pbuf, drecv, mine, ysend, yrecv, gbuf, xs, xr, wb, zs, zr, zm,
    in_sem, w_sem, ag_recv, agx_send, agz_send, d_send, d_recv, y_send, y_recv,
    gy_send, gy_recv, gd_send, gd_recv, x_send, x_recv, z_send, z_recv, zm_recv,
):
    gx, gy, gz = lax.axis_index("gx"), lax.axis_index("gy"), lax.axis_index("gz")
    where_y, core = gy // 2, gy % 2
    mate = gy + 1 - 2 * core
    over = gy + 2 - 4 * where_y
    across = 1 - gx
    near = gz + 1 - 2 * (gz % 2)
    middle = (gz == 1) | (gz == 2)
    both = 2 * rows
    quarter = width // QUARTERS
    piece = depth // PIECES

    def remote(src, dst, send, recv, **where):
        return pltpu.make_async_remote_copy(
            src_ref=src, dst_ref=dst, send_sem=send, recv_sem=recv,
            device_id=where, device_id_type=MESH,
        )

    def slot(j):
        return pl.ds(pl.multiple_of(j * rows, 16), rows)

    def columns(q):
        return pl.ds(pl.multiple_of(q * quarter, 128), quarter)

    def gather_x(k):
        return remote(
            xbuf.at[:, slot(2 * k + 1), :], xbuf.at[:, slot(2 * k + 2), :],
            agx_send.at[k], ag_recv.at[2 * k + 2], gx=across,
        )

    def gather_z(src, dst, way, n, to):
        return remote(
            xbuf.at[:, slot(src), :], xbuf.at[:, slot(dst), :],
            agz_send.at[way, n], ag_recv.at[dst], gz=to,
        )

    def mate_sums(s, t):
        return remote(
            pbuf.at[t], drecv.at[s % 2, t], d_send.at[t], d_recv.at[s % 2, t], gy=mate
        )

    def over_sums(s, h):
        part = pl.ds(h * rows, rows)
        return remote(
            ysend.at[s, :, part, :], yrecv.at[s, :, part, :],
            y_send.at[s, h], y_recv.at[s, h], gy=over,
        )

    def over_grads(j, q):
        block = gbuf.at[:, slot(j), columns(q)]
        return remote(block, block, gy_send.at[j], gy_recv.at[j], gy=over)

    def mate_grads(j, q, n):
        block = gbuf.at[:, slot(j), columns(q)]
        return remote(block, block, gd_send.at[j, n], gd_recv.at[j, n], gy=mate)

    def out_x(k, n):
        return remote(xs.at[k, n], xr.at[k, n], x_send.at[k, n], x_recv.at[k, n], gx=across)

    def to_owner(k, n, lane, to):
        return remote(zs.at[k, n], zr.at[lane, n], z_send.at[k, n], z_recv.at[lane, n], gz=to)

    def to_middle(k, n):
        return remote(
            zs.at[k, n], zm.at[k - 2, n], z_send.at[k, n], zm_recv.at[k - 2, n], gz=near
        )

    def quarter_of(t):
        y_of = where_y + (1 - t % 2) * (1 - 2 * where_y)
        core_of = core + (1 - t // 2) * (1 - 2 * core)
        return 2 * y_of + core_of

    def load_weights(t):
        q = quarter_of(t)
        return [
            pltpu.make_async_copy(gw_hbm.at[:, columns(q)], gw.at[:, columns(q)], w_sem.at[0, t]),
            pltpu.make_async_copy(uw_hbm.at[:, columns(q)], uw.at[:, columns(q)], w_sem.at[1, t]),
            pltpu.make_async_copy(dw_hbm.at[columns(q), :], dw.at[columns(q), :], w_sem.at[2, t]),
        ]

    load_in = [
        pltpu.make_async_copy(ref, xbuf.at[i, slot(1), :], in_sem.at[i])
        for i, ref in enumerate((x_hbm, og_hbm))
    ]
    for copy in load_in:
        copy.start()

    barrier = pltpu.get_barrier_semaphore()
    pl.semaphore_signal(barrier, inc=1, device_id={"gy": mate}, device_id_type=MESH)
    pl.semaphore_signal(barrier, inc=1, device_id={"gy": over}, device_id_type=MESH)
    pl.semaphore_signal(barrier, inc=1, device_id={"gx": across}, device_id_type=MESH)
    for step in range(1, 4):
        pl.semaphore_signal(
            barrier, inc=1, device_id={"gz": (gz + step) % 4}, device_id_type=MESH
        )
    for copy in load_in:
        copy.wait()
    for t in range(QUARTERS):
        for copy in load_weights(t):
            copy.start()
    pl.semaphore_wait(barrier, 6)

    def landing(to, src):
        return 2 * ORDER[to].index(src) + 3

    def z_sends(z, first):
        copies = []
        for way, step in ((0, 1), (1, -1)):
            if not 0 <= z + step < 4:
                continue
            n = 0
            src = z
            while 0 <= src < 4:
                from_slot = 1 if src == z else landing(z, src)
                wave = abs(src - z)
                if wave in first:
                    copies.append(gather_z(from_slot, landing(z + step, src), way, n, z + step))
                n += 1
                src -= step
        return copies

    def at_place(z):
        return pl.when(gz == z)

    gather_x(0).start()
    for z in range(4):
        @at_place(z)
        def _(z=z):
            for copy in z_sends(z, (0,)):
                copy.start()

    def arrive(k):
        slot_k = 2 * k + 1
        gather_z(1, slot_k, 0, 0, 0 * gz).wait_recv()

    def forward_step(s):
        for z in range(4):
            @at_place(z)
            def _(z=z):
                middle = z in (1, 2)
                waits = {1: (1, 2), 2: (3,), 3: ()}[s] if middle else (s,)
                for k in waits:
                    arrive(k)
                for copy in z_sends(z, (s,)):
                    copy.start()
                for k in waits:
                    gather_x(k).start()

    def has_first(s):
        return s >= 1

    def has_second(s):
        return s <= CHUNKS - 2

    def each_half(s, act):
        pl.when(has_first(s))(lambda: act(0))
        pl.when(has_second(s))(lambda: act(1))

    def project(s):
        @pl.when(s >= 1)
        def _():
            gather_x(s - 1).wait_recv()
            for t in range(2):
                mate_sums(s - 1, t).wait_send()

        chunk = pl.ds(pl.multiple_of(s * both, 16), both)

        def one(t, carry):
            q = quarter_of(t)

            @pl.when(s == 0)
            def _():
                for copy in load_weights(t):
                    copy.wait()

            x = xbuf[0, chunk, :]
            pbuf[t, 0] = jnp.dot(x, gw[:, columns(q)], preferred_element_type=F32)
            pbuf[t, 1] = jnp.dot(x, uw[:, columns(q)], preferred_element_type=F32)
            pbuf[t, 2] = contract_last(xbuf[1, chunk, :], dw[columns(q), :])

            @pl.when(t < 2)
            def _():
                mate_sums(s, t).start()

            @pl.when(t == 2)
            def _():
                mate_sums(s, 0).wait_recv()

                def add(r, carry):
                    part = pl.ds(pl.multiple_of(r * 16, 16), 16)
                    for i in range(3):
                        total = pbuf[2, i, part, :] + drecv[s % 2, 0, i, part, :]
                        ysend[s, i, part, :] = total.astype(BF16)
                    return carry

                lax.fori_loop(0, both // 16, add, 0)
                each_half(s, lambda h: over_sums(s, h).start())

            @pl.when(t == 3)
            def _():
                mate_sums(s, 1).wait_recv()

                def add(r, carry):
                    part = pl.ds(pl.multiple_of(r * 16, 16), 16)
                    for i in range(3):
                        mine[s % 2, i, part, :] = pbuf[3, i, part, :] + drecv[s % 2, 1, i, part, :]
                    return carry

                lax.fori_loop(0, both // 16, add, 0)

            return carry

        lax.fori_loop(0, QUARTERS, one, 0)

    def differentiate(s):
        each_half(s, lambda h: over_sums(s, h).wait_recv())

        def block(r, carry):
            part = pl.ds(pl.multiple_of(r * 16, 16), 16)
            terms = [mine[s % 2, i, part, :] + yrecv[s, i, part, :].astype(F32) for i in range(3)]
            here = pl.ds(pl.multiple_of(s * both + r * 16, 16), 16)
            gbuf[0, here, columns(gy)], gbuf[1, here, columns(gy)] = grads_of(*terms)
            return carry

        lax.fori_loop(0, both // 16, block, 0)
        each_half(s, lambda h: mate_grads(2 * s + h, gy, 0).start())

    def hand_over(*slots):
        for j in slots:
            over_grads(j, gy).start()

    def backproject(k, s):
        for h in (1, 2):
            over_grads(2 * k + h, over).wait_recv()
            mate_grads(2 * k + h, over, 1).start()
        for h in (1, 2):
            mate_grads(2 * k + h, mate, 0).wait_recv()
            mate_grads(2 * k + h, mate + over - gy, 1).wait_recv()
        pair = pl.ds(pl.multiple_of((2 * k + 1) * rows, 16), both)

        def one(n, carry):
            here = pl.ds(pl.multiple_of(n * piece, 128), piece)
            part = contract_last(gbuf[0, pair, :], gw[here, :])
            part = part + contract_last(gbuf[1, pair, :], uw[here, :])
            xs[k, n] = part[rows:].astype(BF16)
            wb[k, n] = part[:rows]
            out_x(k, n).start()

            @pl.when((s == 5) & jnp.logical_not(middle))
            def _():
                pass_to_middle(2, n)

            @pl.when(s == 6)
            def _():
                pl.when(middle)(lambda: pass_from_middle(2, n))
                pass_near(n)

            return carry

        lax.fori_loop(0, PIECES, one, 0)

    def paired(k, n):
        out_x(k, n).wait_recv()
        return wb[k, n] + xr[k, n].astype(F32)

    def pass_near(n):
        zs[1, n] = paired(1, n).astype(BF16)
        to_owner(1, n, 0, near).start()

    def pass_to_middle(k, n):
        zs[k, n] = paired(k, n).astype(BF16)
        to_middle(k, n).start()

    def pass_from_middle(k, n):
        total = paired(k, n)
        to_middle(k, n).wait_recv()
        zs[k, n] = (total + zm[k - 2, n].astype(F32)).astype(BF16)
        to_owner(k, n, 1, 3 - gz if k == 2 else (gz + 2) % 4).start()

    def stage(s, carry):
        pl.when(s == 2)(lambda: forward_step(2))
        pl.when(s == 3)(lambda: forward_step(3))

        @pl.when((s == 1) | (s == 2) | (s == 4))
        def _():
            differentiate(s - 1)

        @pl.when(s == 1)
        def _():
            hand_over(1)
            forward_step(1)

        pl.when(s == 2)(lambda: hand_over(2))
        pl.when(s == 4)(lambda: hand_over(6))
        pl.when(s < CHUNKS)(lambda: project(s))
        pl.when(s == 2)(lambda: hand_over(3))

        @pl.when(s == 3)
        def _():
            differentiate(2)
            hand_over(5)

        pl.when(s == 4)(lambda: hand_over(4, 7))

        @pl.when(s >= 3)
        def _():
            backproject(s - 3 + (s == 4).astype(jnp.int32) - (s == 5).astype(jnp.int32), s)

        @pl.when(s == 4)
        def _():
            differentiate(4)
            hand_over(8)

        return carry

    lax.fori_loop(0, CHUNKS + 2, stage, 0)

    def last(n, carry):
        pl.when(middle)(lambda: pass_from_middle(3, n))
        pl.when(jnp.logical_not(middle))(lambda: pass_to_middle(3, n))
        return carry

    lax.fori_loop(0, PIECES, last, 0)

    for n in range(PIECES):
        out_x(0, n).wait_recv()
        total = wb[0, n] + xr[0, n].astype(F32)
        for lane in range(2):
            to_owner(1, n, lane, near).wait_recv()
            total = total + zr[lane, n].astype(F32)
        out_ref[:, n * piece : (n + 1) * piece] = total.astype(BF16)

    for k in range(4):
        gather_x(k).wait_send()
    for z in range(4):
        @at_place(z)
        def _(z=z):
            for copy in z_sends(z, (0, 1, 2)):
                copy.wait_send()
    for t in range(2):
        mate_sums(CHUNKS - 1, t).wait_send()

    def drain_sums(s, carry):
        each_half(s, lambda h: over_sums(s, h).wait_send())
        return carry

    def drain_grads(j, carry):
        over_grads(j, gy).wait_send()
        for n in range(2):
            mate_grads(j, gy, n).wait_send()
        return carry

    def drain_out(k, carry):
        for n in range(PIECES):
            out_x(k, n).wait_send()

        @pl.when(k >= 1)
        def _():
            for n in range(PIECES):
                to_owner(k, n, 0, near).wait_send()

        return carry

    lax.fori_loop(0, CHUNKS, drain_sums, 0)
    lax.fori_loop(1, 2 * CHUNKS - 1, drain_grads, 0)
    lax.fori_loop(0, 4, drain_out, 0)


def fused(inputs, out_grad, gate_weight, up_weight, down_weight):
    rows, depth = inputs.shape
    width = gate_weight.shape[1]
    both, quarter, piece = 2 * rows, width // QUARTERS, depth // PIECES
    dma = pltpu.SemaphoreType.DMA
    n = CHUNKS
    scratch = [
        pltpu.VMEM((2, n * both, depth), BF16),
        pltpu.VMEM((depth, width), BF16),
        pltpu.VMEM((depth, width), BF16),
        pltpu.VMEM((width, depth), BF16),
        pltpu.VMEM((4, 3, both, quarter), F32),
        pltpu.VMEM((2, 2, 3, both, quarter), F32),
        pltpu.VMEM((2, 3, both, quarter), F32),
        pltpu.VMEM((n, 3, both, quarter), BF16),
        pltpu.VMEM((n, 3, both, quarter), BF16),
        pltpu.VMEM((2, n * both, width), BF16),
        pltpu.VMEM((4, PIECES, rows, piece), BF16),
        pltpu.VMEM((4, PIECES, rows, piece), BF16),
        pltpu.VMEM((4, PIECES, rows, piece), F32),
        pltpu.VMEM((4, PIECES, rows, piece), BF16),
        pltpu.VMEM((2, PIECES, rows, piece), BF16),
        pltpu.VMEM((2, PIECES, rows, piece), BF16),
        dma((2,)), dma((3, 4)), dma((2 * n,)), dma((4,)), dma((2, 4)), dma((2,)), dma((2, 2)),
        dma((n, 2)), dma((n, 2)), dma((2 * n,)), dma((2 * n,)), dma((2 * n, 2)), dma((2 * n, 2)),
        dma((4, PIECES)), dma((4, PIECES)), dma((4, PIECES)), dma((2, PIECES)), dma((2, PIECES)),
    ]
    return pl.pallas_call(
        functools.partial(kernel, rows, depth, width),
        out_shape=jax.ShapeDtypeStruct((rows, depth), BF16),
        in_specs=[pl.BlockSpec(memory_space=pl.ANY)] * 5,
        out_specs=pl.BlockSpec(memory_space=pltpu.VMEM),
        scratch_shapes=scratch,
        compiler_params=pltpu.CompilerParams(
            collective_id=0, has_side_effects=True, vmem_limit_bytes=66 * 1024 * 1000
        ),
    )(inputs, out_grad, gate_weight, up_weight, down_weight)


def plain(nx, ny, nz):
    def layer(inputs, out_grad, gate_weight, up_weight, down_weight):
        both = lax.all_gather(jnp.stack([inputs, out_grad]), ("gx", "gz"), axis=1, tiled=True)
        gate = jnp.dot(both[0], gate_weight, preferred_element_type=F32)
        upper = jnp.dot(both[0], up_weight, preferred_element_type=F32)
        hidden = contract_last(both[1], down_weight)
        terms = lax.psum_scatter(
            jnp.stack([gate, upper, hidden]), "gy", scatter_dimension=1, tiled=True
        )
        grads = jnp.stack(grads_of(terms[0], terms[1], terms[2]))
        grads = lax.all_gather(grads, "gy", axis=1, tiled=True)
        total = contract_last(grads[0], gate_weight) + contract_last(grads[1], up_weight)
        total = lax.psum_scatter(total, ("gx", "gz"), scatter_dimension=0, tiled=True)
        return total.astype(BF16)

    return layer


def solution(mesh):
    nx, ny, nz = mesh.shape["gx"], mesh.shape["gy"], mesh.shape["gz"]
    body = fused if (nx, ny, nz) == (2, 4, 4) else plain(nx, ny, nz)
    return jax.shard_map(body, mesh=mesh, in_specs=SPECS, out_specs=OUT_SPEC, check_vma=False)
```

```python
import functools

import jax
import jax.numpy as jnp
from jax import lax
from jax.experimental import pallas as pl
from jax.experimental.pallas import tpu as pltpu
from jax.sharding import PartitionSpec as P

F32, BF16 = jnp.float32, jnp.bfloat16
MESH = pl.DeviceIdType.MESH
SPECS = (
    P(("gx", "gz"), "gy"),
    P(("gx", "gz"), "gy"),
    P("gy", ("gx", "gz")),
    P("gy", ("gx", "gz")),
    P(("gx", "gz"), "gy"),
)
OUT_SPEC = P(("gx", "gz"), "gy")


def contract_last(left, right):
    return lax.dot_general(left, right, (((1,), (1,)), ((), ())), preferred_element_type=F32)


def grads_of(gate, upper, hidden_grad):
    logistic = jax.nn.sigmoid(gate)
    gate_grad = hidden_grad * upper * logistic * (1.0 + gate * (1.0 - logistic))
    up_grad = hidden_grad * gate * logistic
    return gate_grad.astype(BF16), up_grad.astype(BF16)


ORDER = {0: (1, 2, 3), 1: (0, 2, 3), 2: (3, 1, 0), 3: (2, 1, 0)}
CHUNKS = 5
QUARTERS = 4
PIECES = 4
SENDS = 8


def kernel(
    rows, depth, width,
    x_hbm, og_hbm, gw_hbm, uw_hbm, dw_hbm, out_ref,
    xbuf, gw, uw, dw, pbuf, drecv, mine, ysend, yrecv, gbuf, xs, xr, wb, zs, zr, zm,
    in_sem, w_sem, ag_recv, agx_send, agz_send, d_send, d_recv, y_send, y_recv,
    gy_send, gy_recv, gd_send, gd_recv, x_send, x_recv, z_send, z_recv, zm_recv, obuf, o_sem,
):
    gx, gy, gz = lax.axis_index("gx"), lax.axis_index("gy"), lax.axis_index("gz")
    where_y, core = gy // 2, gy % 2
    mate = gy + 1 - 2 * core
    over = gy + 2 - 4 * where_y
    across = 1 - gx
    near = gz + 1 - 2 * (gz % 2)
    middle = (gz == 1) | (gz == 2)
    both = 2 * rows
    quarter = width // QUARTERS
    piece, strip = depth // PIECES, depth // SENDS
    per = SENDS // PIECES

    def remote(src, dst, send, recv, **where):
        return pltpu.make_async_remote_copy(
            src_ref=src, dst_ref=dst, send_sem=send, recv_sem=recv,
            device_id=where, device_id_type=MESH,
        )

    def slot(j):
        return pl.ds(pl.multiple_of(j * rows, 16), rows)

    def columns(q):
        return pl.ds(pl.multiple_of(q * quarter, 128), quarter)

    def gather_x(k):
        return remote(
            xbuf.at[:, slot(2 * k + 1), :], xbuf.at[:, slot(2 * k + 2), :],
            agx_send.at[k], ag_recv.at[2 * k + 2], gx=across,
        )

    def gather_z(src, dst, way, n, to):
        return remote(
            xbuf.at[:, slot(src), :], xbuf.at[:, slot(dst), :],
            agz_send.at[way, n], ag_recv.at[dst], gz=to,
        )

    def mate_sums(s, t):
        return remote(
            pbuf.at[t], drecv.at[s % 2, t], d_send.at[t], d_recv.at[s % 2, t], gy=mate
        )

    def over_sums(s, h):
        part = pl.ds(h * rows, rows)
        return remote(
            ysend.at[s, :, part, :], yrecv.at[s, :, part, :],
            y_send.at[s, h], y_recv.at[s, h], gy=over,
        )

    def over_grads(j, q):
        block = gbuf.at[:, slot(j), columns(q)]
        return remote(block, block, gy_send.at[j], gy_recv.at[j], gy=over)

    def mate_grads(j, q, n):
        block = gbuf.at[:, slot(j), columns(q)]
        return remote(block, block, gd_send.at[j, n], gd_recv.at[j, n], gy=mate)

    def out_x(k, n):
        return remote(xs.at[k, n], xr.at[k, n], x_send.at[k, n], x_recv.at[k, n], gx=across)

    def to_owner(k, n, lane, to):
        return remote(zs.at[k, n], zr.at[lane, n], z_send.at[k, n], z_recv.at[lane, n], gz=to)

    def to_middle(k, n):
        return remote(
            zs.at[k, n], zm.at[k - 2, n], z_send.at[k, n], zm_recv.at[k - 2, n], gz=near
        )

    def quarter_of(t):
        y_of = where_y + (1 - t % 2) * (1 - 2 * where_y)
        core_of = core + (1 - t // 2) * (1 - 2 * core)
        return 2 * y_of + core_of

    def load_weights(t):
        q = quarter_of(t)
        return [
            pltpu.make_async_copy(gw_hbm.at[:, columns(q)], gw.at[:, columns(q)], w_sem.at[0, t]),
            pltpu.make_async_copy(uw_hbm.at[:, columns(q)], uw.at[:, columns(q)], w_sem.at[1, t]),
            pltpu.make_async_copy(dw_hbm.at[columns(q), :], dw.at[columns(q), :], w_sem.at[2, t]),
        ]

    load_in = [
        pltpu.make_async_copy(ref, xbuf.at[i, slot(1), :], in_sem.at[i])
        for i, ref in enumerate((x_hbm, og_hbm))
    ]
    for copy in load_in:
        copy.start()

    barrier = pltpu.get_barrier_semaphore()
    pl.semaphore_signal(barrier, inc=1, device_id={"gy": mate}, device_id_type=MESH)
    pl.semaphore_signal(barrier, inc=1, device_id={"gy": over}, device_id_type=MESH)
    pl.semaphore_signal(barrier, inc=1, device_id={"gx": across}, device_id_type=MESH)
    for step in range(1, 4):
        pl.semaphore_signal(
            barrier, inc=1, device_id={"gz": (gz + step) % 4}, device_id_type=MESH
        )
    for copy in load_in:
        copy.wait()
    for t in range(QUARTERS):
        for copy in load_weights(t):
            copy.start()
    pl.semaphore_wait(barrier, 6)

    def landing(to, src):
        return 2 * ORDER[to].index(src) + 3

    def z_sends(z, first):
        copies = []
        for way, step in ((0, 1), (1, -1)):
            if not 0 <= z + step < 4:
                continue
            n = 0
            src = z
            while 0 <= src < 4:
                from_slot = 1 if src == z else landing(z, src)
                wave = abs(src - z)
                if wave in first:
                    copies.append(gather_z(from_slot, landing(z + step, src), way, n, z + step))
                n += 1
                src -= step
        return copies

    def at_place(z):
        return pl.when(gz == z)

    gather_x(0).start()
    for z in range(4):
        @at_place(z)
        def _(z=z):
            for copy in z_sends(z, (0,)):
                copy.start()

    def arrive(k):
        slot_k = 2 * k + 1
        gather_z(1, slot_k, 0, 0, 0 * gz).wait_recv()

    def forward_step(s):
        for z in range(4):
            @at_place(z)
            def _(z=z):
                middle = z in (1, 2)
                waits = {1: (1, 2), 2: (3,), 3: ()}[s] if middle else (s,)
                for k in waits:
                    arrive(k)
                for copy in z_sends(z, (s,)):
                    copy.start()
                for k in waits:
                    gather_x(k).start()

    def has_first(s):
        return s >= 1

    def has_second(s):
        return s <= CHUNKS - 2

    def each_half(s, act):
        pl.when(has_first(s))(lambda: act(0))
        pl.when(has_second(s))(lambda: act(1))

    def project(s):
        @pl.when(s >= 1)
        def _():
            gather_x(s - 1).wait_recv()
            for t in range(2):
                mate_sums(s - 1, t).wait_send()

        chunk = pl.ds(pl.multiple_of(s * both, 16), both)

        def one(t, carry):
            q = quarter_of(t)

            @pl.when(s == 0)
            def _():
                for copy in load_weights(t):
                    copy.wait()

            x = xbuf[0, chunk, :]
            pbuf[t, 0] = jnp.dot(x, gw[:, columns(q)], preferred_element_type=F32)
            pbuf[t, 1] = jnp.dot(x, uw[:, columns(q)], preferred_element_type=F32)
            pbuf[t, 2] = contract_last(xbuf[1, chunk, :], dw[columns(q), :])

            @pl.when(t < 2)
            def _():
                mate_sums(s, t).start()

            @pl.when(t == 2)
            def _():
                mate_sums(s, 0).wait_recv()

                def add(r, carry):
                    part = pl.ds(pl.multiple_of(r * 16, 16), 16)
                    for i in range(3):
                        total = pbuf[2, i, part, :] + drecv[s % 2, 0, i, part, :]
                        ysend[s, i, part, :] = total.astype(BF16)
                    return carry

                lax.fori_loop(0, both // 16, add, 0)
                each_half(s, lambda h: over_sums(s, h).start())

            @pl.when(t == 3)
            def _():
                mate_sums(s, 1).wait_recv()

                def add(r, carry):
                    part = pl.ds(pl.multiple_of(r * 16, 16), 16)
                    for i in range(3):
                        mine[s % 2, i, part, :] = pbuf[3, i, part, :] + drecv[s % 2, 1, i, part, :]
                    return carry

                lax.fori_loop(0, both // 16, add, 0)

            return carry

        lax.fori_loop(0, QUARTERS, one, 0)

    def differentiate(s):
        each_half(s, lambda h: over_sums(s, h).wait_recv())

        def block(r, carry):
            part = pl.ds(pl.multiple_of(r * 16, 16), 16)
            terms = [mine[s % 2, i, part, :] + yrecv[s, i, part, :].astype(F32) for i in range(3)]
            here = pl.ds(pl.multiple_of(s * both + r * 16, 16), 16)
            gbuf[0, here, columns(gy)], gbuf[1, here, columns(gy)] = grads_of(*terms)
            return carry

        lax.fori_loop(0, both // 16, block, 0)
        each_half(s, lambda h: mate_grads(2 * s + h, gy, 0).start())

    def hand_over(*slots):
        for j in slots:
            over_grads(j, gy).start()

    def backproject(k, s):
        for h in (1, 2):
            over_grads(2 * k + h, over).wait_recv()
            mate_grads(2 * k + h, over, 1).start()
        for h in (1, 2):
            mate_grads(2 * k + h, mate, 0).wait_recv()
            mate_grads(2 * k + h, mate + over - gy, 1).wait_recv()
        pair = pl.ds(pl.multiple_of((2 * k + 1) * rows, 16), both)

        def one(n, carry):
            here = pl.ds(pl.multiple_of(n * piece, 128), piece)
            part = contract_last(gbuf[0, pair, :], gw[here, :])
            part = part + contract_last(gbuf[1, pair, :], uw[here, :])
            for i in range(per):
                m = n * per + i
                xs[k, m] = part[rows:, i * strip : (i + 1) * strip].astype(BF16)
                wb[k, m] = part[:rows, i * strip : (i + 1) * strip]
                out_x(k, m).start()

            pl.when((s == 5) & middle)(lambda: from_middle(2, n))
            pl.when((s == 5) & (n < 2) & jnp.logical_not(middle))(lambda: into_middle(2, n + 2))
            pl.when((s == 6) & (n < 2))(lambda: to_near(n + 2))
            pl.when((s == 6) & (n >= 2) & jnp.logical_not(middle))(lambda: into_middle(3, n - 2))
            return carry

        lax.fori_loop(0, PIECES, one, 0)

    def to_near(n):
        for i in range(per):
            pass_near(n * per + i)

    def into_middle(k, n):
        for i in range(per):
            pass_to_middle(k, n * per + i)

    def from_middle(k, n):
        for i in range(per):
            pass_from_middle(k, n * per + i)

    def paired(k, n):
        out_x(k, n).wait_recv()
        return wb[k, n] + xr[k, n].astype(F32)

    def pass_near(n):
        zs[1, n] = paired(1, n).astype(BF16)
        to_owner(1, n, 0, near).start()

    def pass_to_middle(k, n):
        zs[k, n] = paired(k, n).astype(BF16)
        to_middle(k, n).start()

    def pass_from_middle(k, n):
        total = paired(k, n)
        to_middle(k, n).wait_recv()
        zs[k, n] = (total + zm[k - 2, n].astype(F32)).astype(BF16)
        to_owner(k, n, 1, 3 - gz if k == 2 else (gz + 2) % 4).start()

    def stage(s, carry):
        pl.when(s == 2)(lambda: forward_step(2))
        pl.when(s == 3)(lambda: forward_step(3))

        @pl.when((s == 1) | (s == 2) | (s == 4))
        def _():
            differentiate(s - 1)

        @pl.when(s == 1)
        def _():
            hand_over(1)
            forward_step(1)

        pl.when(s == 2)(lambda: hand_over(2))
        pl.when(s == 4)(lambda: hand_over(6))
        pl.when(s < CHUNKS)(lambda: project(s))
        pl.when(s == 2)(lambda: hand_over(3))

        @pl.when(s == 3)
        def _():
            differentiate(2)
            hand_over(5)

        pl.when(s == 4)(lambda: hand_over(4, 7))

        @pl.when(s >= 3)
        def _():
            pair = jnp.where(s == 4, 2, jnp.where(s == 5, 1, s - 3))
            backproject(pair, s)

        @pl.when(s == 4)
        def _():
            differentiate(4)
            hand_over(8)

            @pl.when(jnp.logical_not(middle))
            def _():
                for n in range(2):
                    into_middle(2, n)

        @pl.when(s == 5)
        def _():
            for n in range(2):
                to_near(n)

        return carry

    lax.fori_loop(0, CHUNKS + 2, stage, 0)

    @pl.when(middle)
    def _():
        for n in range(PIECES):
            from_middle(3, n)

    @pl.when(jnp.logical_not(middle))
    def _():
        for n in (PIECES - 2, PIECES - 1):
            into_middle(3, n)

    def out_copy(n):
        return pltpu.make_async_copy(
            obuf.at[n], out_ref.at[:, pl.ds(pl.multiple_of(n * strip, 128), strip)], o_sem.at[n]
        )

    def finish(n, carry):
        out_x(0, n).wait_recv()
        total = wb[0, n] + xr[0, n].astype(F32)
        for lane in range(2):
            to_owner(1, n, lane, near).wait_recv()
            total = total + zr[lane, n].astype(F32)
        obuf[n] = total.astype(BF16)
        out_copy(n).start()
        return carry

    lax.fori_loop(0, SENDS, finish, 0)

    for k in range(4):
        gather_x(k).wait_send()
    for z in range(4):
        @at_place(z)
        def _(z=z):
            for copy in z_sends(z, (0, 1, 2)):
                copy.wait_send()
    for t in range(2):
        mate_sums(CHUNKS - 1, t).wait_send()

    def drain_sums(s, carry):
        each_half(s, lambda h: over_sums(s, h).wait_send())
        return carry

    def drain_grads(j, carry):
        over_grads(j, gy).wait_send()
        for n in range(2):
            mate_grads(j, gy, n).wait_send()
        return carry

    def drain_out(k, carry):
        for n in range(SENDS):
            out_x(k, n).wait_send()

        @pl.when(k >= 1)
        def _():
            for n in range(SENDS):
                to_owner(k, n, 0, near).wait_send()

        return carry

    lax.fori_loop(0, CHUNKS, drain_sums, 0)
    lax.fori_loop(1, 2 * CHUNKS - 1, drain_grads, 0)
    lax.fori_loop(0, 4, drain_out, 0)
    for n in range(SENDS):
        out_copy(n).wait()


def fused(inputs, out_grad, gate_weight, up_weight, down_weight):
    rows, depth = inputs.shape
    width = gate_weight.shape[1]
    both, quarter, strip = 2 * rows, width // QUARTERS, depth // SENDS
    dma = pltpu.SemaphoreType.DMA
    n = CHUNKS
    scratch = [
        pltpu.VMEM((2, n * both, depth), BF16),
        pltpu.VMEM((depth, width), BF16),
        pltpu.VMEM((depth, width), BF16),
        pltpu.VMEM((width, depth), BF16),
        pltpu.VMEM((4, 3, both, quarter), F32),
        pltpu.VMEM((2, 2, 3, both, quarter), F32),
        pltpu.VMEM((2, 3, both, quarter), F32),
        pltpu.VMEM((n, 3, both, quarter), BF16),
        pltpu.VMEM((n, 3, both, quarter), BF16),
        pltpu.VMEM((2, n * both, width), BF16),
        pltpu.VMEM((4, SENDS, rows, strip), BF16),
        pltpu.VMEM((4, SENDS, rows, strip), BF16),
        pltpu.VMEM((4, SENDS, rows, strip), F32),
        pltpu.VMEM((4, SENDS, rows, strip), BF16),
        pltpu.VMEM((2, SENDS, rows, strip), BF16),
        pltpu.VMEM((2, SENDS, rows, strip), BF16),
        dma((2,)), dma((3, 4)), dma((2 * n,)), dma((4,)), dma((2, 4)), dma((2,)), dma((2, 2)),
        dma((n, 2)), dma((n, 2)), dma((2 * n,)), dma((2 * n,)), dma((2 * n, 2)), dma((2 * n, 2)),
        dma((4, SENDS)), dma((4, SENDS)), dma((4, SENDS)), dma((2, SENDS)), dma((2, SENDS)),
        pltpu.VMEM((SENDS, rows, strip), BF16), dma((SENDS,)),
    ]
    return pl.pallas_call(
        functools.partial(kernel, rows, depth, width),
        out_shape=jax.ShapeDtypeStruct((rows, depth), BF16),
        in_specs=[pl.BlockSpec(memory_space=pl.ANY)] * 5,
        out_specs=pl.BlockSpec(memory_space=pl.ANY),
        scratch_shapes=scratch,
        compiler_params=pltpu.CompilerParams(
            collective_id=0, has_side_effects=True, vmem_limit_bytes=66 * 1024 * 1000
        ),
    )(inputs, out_grad, gate_weight, up_weight, down_weight)


def plain(nx, ny, nz):
    def layer(inputs, out_grad, gate_weight, up_weight, down_weight):
        both = lax.all_gather(jnp.stack([inputs, out_grad]), ("gx", "gz"), axis=1, tiled=True)
        gate = jnp.dot(both[0], gate_weight, preferred_element_type=F32)
        upper = jnp.dot(both[0], up_weight, preferred_element_type=F32)
        hidden = contract_last(both[1], down_weight)
        terms = lax.psum_scatter(
            jnp.stack([gate, upper, hidden]), "gy", scatter_dimension=1, tiled=True
        )
        grads = jnp.stack(grads_of(terms[0], terms[1], terms[2]))
        grads = lax.all_gather(grads, "gy", axis=1, tiled=True)
        total = contract_last(grads[0], gate_weight) + contract_last(grads[1], up_weight)
        total = lax.psum_scatter(total, ("gx", "gz"), scatter_dimension=0, tiled=True)
        return total.astype(BF16)

    return layer


def solution(mesh):
    nx, ny, nz = mesh.shape["gx"], mesh.shape["gy"], mesh.shape["gz"]
    body = fused if (nx, ny, nz) == (2, 4, 4) else plain(nx, ny, nz)
    return jax.shard_map(body, mesh=mesh, in_specs=SPECS, out_specs=OUT_SPEC, check_vma=False)
```

```python
import functools

import jax
import jax.numpy as jnp
from jax import lax
from jax.experimental import pallas as pl
from jax.experimental.pallas import tpu as pltpu
from jax.sharding import PartitionSpec as P

F32, BF16 = jnp.float32, jnp.bfloat16
MESH = pl.DeviceIdType.MESH
SPECS = (
    P(("gx", "gz"), "gy"),
    P(("gx", "gz"), "gy"),
    P("gy", ("gx", "gz")),
    P("gy", ("gx", "gz")),
    P(("gx", "gz"), "gy"),
)
OUT_SPEC = P(("gx", "gz"), "gy")


def contract_last(left, right):
    return lax.dot_general(left, right, (((1,), (1,)), ((), ())), preferred_element_type=F32)


def grads_of(gate, upper, hidden_grad):
    logistic = jax.nn.sigmoid(gate)
    gate_grad = hidden_grad * upper * logistic * (1.0 + gate * (1.0 - logistic))
    up_grad = hidden_grad * gate * logistic
    return gate_grad.astype(BF16), up_grad.astype(BF16)


ORDER = {0: (1, 2, 3), 1: (0, 2, 3), 2: (3, 1, 0), 3: (2, 1, 0)}
CHUNKS = 5
QUARTERS = 4
PIECES = 4
SENDS = 8


def kernel(
    rows, depth, width,
    x_hbm, og_hbm, gw_hbm, uw_hbm, dw_hbm, out_ref,
    xbuf, gw, uw, dw, pbuf, drecv, mine, ysend, yrecv, gbuf, xs, xr, wb, zs, zr, zm,
    in_sem, w_sem, ag_recv, agx_send, agz_send, d_send, d_recv, y_send, y_recv,
    gy_send, gy_recv, gd_send, gd_recv, x_send, x_recv, z_send, z_recv, zm_recv, obuf, o_sem,
):
    gx, gy, gz = lax.axis_index("gx"), lax.axis_index("gy"), lax.axis_index("gz")
    where_y, core = gy // 2, gy % 2
    mate = gy + 1 - 2 * core
    over = gy + 2 - 4 * where_y
    across = 1 - gx
    near = gz + 1 - 2 * (gz % 2)
    middle = (gz == 1) | (gz == 2)
    both = 2 * rows
    quarter = width // QUARTERS
    piece, strip = depth // PIECES, depth // SENDS
    per = SENDS // PIECES

    def remote(src, dst, send, recv, **where):
        return pltpu.make_async_remote_copy(
            src_ref=src, dst_ref=dst, send_sem=send, recv_sem=recv,
            device_id=where, device_id_type=MESH,
        )

    def slot(j):
        return pl.ds(pl.multiple_of(j * rows, 16), rows)

    def columns(q):
        return pl.ds(pl.multiple_of(q * quarter, 128), quarter)

    def gather_x(k):
        return remote(
            xbuf.at[:, slot(2 * k + 1), :], xbuf.at[:, slot(2 * k + 2), :],
            agx_send.at[k], ag_recv.at[2 * k + 2], gx=across,
        )

    def gather_z(src, dst, way, n, to):
        return remote(
            xbuf.at[:, slot(src), :], xbuf.at[:, slot(dst), :],
            agz_send.at[way, n], ag_recv.at[dst], gz=to,
        )

    def mate_sums(s, t):
        return remote(
            pbuf.at[t], drecv.at[s % 2, t], d_send.at[t], d_recv.at[s % 2, t], gy=mate
        )

    def over_sums(s, h):
        part = pl.ds(h * rows, rows)
        return remote(
            ysend.at[s, :, part, :], yrecv.at[s, :, part, :],
            y_send.at[s, h], y_recv.at[s, h], gy=over,
        )

    def over_grads(j, q):
        block = gbuf.at[:, slot(j), columns(q)]
        return remote(block, block, gy_send.at[j], gy_recv.at[j], gy=over)

    def mate_grads(j, q, n):
        block = gbuf.at[:, slot(j), columns(q)]
        return remote(block, block, gd_send.at[j, n], gd_recv.at[j, n], gy=mate)

    def out_x(k, n):
        return remote(xs.at[k, n], xr.at[k, n], x_send.at[k, n], x_recv.at[k, n], gx=across)

    def to_owner(k, n, lane, to):
        return remote(zs.at[k, n], zr.at[lane, n], z_send.at[k, n], z_recv.at[lane, n], gz=to)

    def to_middle(k, n):
        return remote(
            zs.at[k, n], zm.at[k - 2, n], z_send.at[k, n], zm_recv.at[k - 2, n], gz=near
        )

    def quarter_of(t):
        y_of = where_y + (1 - t % 2) * (1 - 2 * where_y)
        core_of = core + (1 - t // 2) * (1 - 2 * core)
        return 2 * y_of + core_of

    def load_weights(t):
        q = quarter_of(t)
        return [
            pltpu.make_async_copy(gw_hbm.at[:, columns(q)], gw.at[:, columns(q)], w_sem.at[0, t]),
            pltpu.make_async_copy(uw_hbm.at[:, columns(q)], uw.at[:, columns(q)], w_sem.at[1, t]),
            pltpu.make_async_copy(dw_hbm.at[columns(q), :], dw.at[columns(q), :], w_sem.at[2, t]),
        ]

    load_in = [
        pltpu.make_async_copy(ref, xbuf.at[i, slot(1), :], in_sem.at[i])
        for i, ref in enumerate((x_hbm, og_hbm))
    ]
    for copy in load_in:
        copy.start()

    barrier = pltpu.get_barrier_semaphore()
    pl.semaphore_signal(barrier, inc=1, device_id={"gy": mate}, device_id_type=MESH)
    pl.semaphore_signal(barrier, inc=1, device_id={"gy": over}, device_id_type=MESH)
    pl.semaphore_signal(barrier, inc=1, device_id={"gx": across}, device_id_type=MESH)
    for step in range(1, 4):
        pl.semaphore_signal(
            barrier, inc=1, device_id={"gz": (gz + step) % 4}, device_id_type=MESH
        )
    for copy in load_in:
        copy.wait()
    for t in range(QUARTERS):
        for copy in load_weights(t):
            copy.start()
    pl.semaphore_wait(barrier, 6)

    def landing(to, src):
        return 2 * ORDER[to].index(src) + 3

    def z_sends(z, first):
        copies = []
        for way, step in ((0, 1), (1, -1)):
            if not 0 <= z + step < 4:
                continue
            n = 0
            src = z
            while 0 <= src < 4:
                from_slot = 1 if src == z else landing(z, src)
                wave = abs(src - z)
                if wave in first:
                    copies.append(gather_z(from_slot, landing(z + step, src), way, n, z + step))
                n += 1
                src -= step
        return copies

    def at_place(z):
        return pl.when(gz == z)

    gather_x(0).start()
    for z in range(4):
        @at_place(z)
        def _(z=z):
            for copy in z_sends(z, (0,)):
                copy.start()

    def arrive(k):
        slot_k = 2 * k + 1
        gather_z(1, slot_k, 0, 0, 0 * gz).wait_recv()

    def forward_step(s):
        for z in range(4):
            @at_place(z)
            def _(z=z):
                middle = z in (1, 2)
                waits = {1: (1, 2), 2: (3,), 3: ()}[s] if middle else (s,)
                for k in waits:
                    arrive(k)
                for copy in z_sends(z, (s,)):
                    copy.start()
                for k in waits:
                    gather_x(k).start()

    def has_first(s):
        return s >= 1

    def has_second(s):
        return s <= CHUNKS - 2

    def each_half(s, act):
        pl.when(has_first(s))(lambda: act(0))
        pl.when(has_second(s))(lambda: act(1))

    def project(s):
        @pl.when(s >= 1)
        def _():
            gather_x(s - 1).wait_recv()
            for t in range(2):
                mate_sums(s - 1, t).wait_send()

        chunk = pl.ds(pl.multiple_of(s * both, 16), both)

        def one(t, carry):
            q = quarter_of(t)

            @pl.when(s == 0)
            def _():
                for copy in load_weights(t):
                    copy.wait()

            x = xbuf[0, chunk, :]
            pbuf[t, 0] = jnp.dot(x, gw[:, columns(q)], preferred_element_type=F32)
            pbuf[t, 1] = jnp.dot(x, uw[:, columns(q)], preferred_element_type=F32)
            pbuf[t, 2] = contract_last(xbuf[1, chunk, :], dw[columns(q), :])

            @pl.when(t < 2)
            def _():
                mate_sums(s, t).start()

            @pl.when(t == 2)
            def _():
                mate_sums(s, 0).wait_recv()

                def add(r, carry):
                    part = pl.ds(pl.multiple_of(r * 16, 16), 16)
                    for i in range(3):
                        total = pbuf[2, i, part, :] + drecv[s % 2, 0, i, part, :]
                        ysend[s, i, part, :] = total.astype(BF16)
                    return carry

                lax.fori_loop(0, both // 16, add, 0)
                each_half(s, lambda h: over_sums(s, h).start())

            @pl.when(t == 3)
            def _():
                mate_sums(s, 1).wait_recv()

                def add(r, carry):
                    part = pl.ds(pl.multiple_of(r * 16, 16), 16)
                    for i in range(3):
                        mine[s % 2, i, part, :] = pbuf[3, i, part, :] + drecv[s % 2, 1, i, part, :]
                    return carry

                lax.fori_loop(0, both // 16, add, 0)

            return carry

        lax.fori_loop(0, QUARTERS, one, 0)

    def differentiate(s):
        each_half(s, lambda h: over_sums(s, h).wait_recv())

        def block(r, carry):
            part = pl.ds(pl.multiple_of(r * 16, 16), 16)
            terms = [mine[s % 2, i, part, :] + yrecv[s, i, part, :].astype(F32) for i in range(3)]
            here = pl.ds(pl.multiple_of(s * both + r * 16, 16), 16)
            gbuf[0, here, columns(gy)], gbuf[1, here, columns(gy)] = grads_of(*terms)
            return carry

        lax.fori_loop(0, both // 16, block, 0)
        each_half(s, lambda h: mate_grads(2 * s + h, gy, 0).start())

    def hand_over(*slots):
        for j in slots:
            over_grads(j, gy).start()

    def backproject(k, s):
        for h in (1, 2):
            over_grads(2 * k + h, over).wait_recv()
            mate_grads(2 * k + h, over, 1).start()
        for h in (1, 2):
            mate_grads(2 * k + h, mate, 0).wait_recv()
            mate_grads(2 * k + h, mate + over - gy, 1).wait_recv()
        pair = pl.ds(pl.multiple_of((2 * k + 1) * rows, 16), both)

        def one(n, carry):
            here = pl.ds(pl.multiple_of(n * piece, 128), piece)
            grads = jnp.concatenate([gbuf[0, pair, :], gbuf[1, pair, :]], axis=1)
            weights = jnp.concatenate([gw[here, :], uw[here, :]], axis=1)
            part = contract_last(grads, weights)
            for i in range(per):
                m = n * per + i
                xs[k, m] = part[rows:, i * strip : (i + 1) * strip].astype(BF16)
                wb[k, m] = part[:rows, i * strip : (i + 1) * strip]
                out_x(k, m).start()

            pl.when((s == 5) & middle)(lambda: from_middle(2, n))
            pl.when((s == 5) & (n < 2) & jnp.logical_not(middle))(lambda: into_middle(2, n + 2))
            pl.when((s == 6) & (n < 2))(lambda: to_near(n + 2))
            pl.when((s == 6) & (n >= 2) & jnp.logical_not(middle))(lambda: into_middle(3, n - 2))
            return carry

        lax.fori_loop(0, PIECES, one, 0)

    def to_near(n):
        for i in range(per):
            pass_near(n * per + i)

    def into_middle(k, n):
        for i in range(per):
            pass_to_middle(k, n * per + i)

    def from_middle(k, n):
        for i in range(per):
            pass_from_middle(k, n * per + i)

    def paired(k, n):
        out_x(k, n).wait_recv()
        return wb[k, n] + xr[k, n].astype(F32)

    def pass_near(n):
        zs[1, n] = paired(1, n).astype(BF16)
        to_owner(1, n, 0, near).start()

    def pass_to_middle(k, n):
        zs[k, n] = paired(k, n).astype(BF16)
        to_middle(k, n).start()

    def pass_from_middle(k, n):
        total = paired(k, n)
        to_middle(k, n).wait_recv()
        zs[k, n] = (total + zm[k - 2, n].astype(F32)).astype(BF16)
        to_owner(k, n, 1, 3 - gz if k == 2 else (gz + 2) % 4).start()

    def stage(s, carry):
        pl.when(s == 2)(lambda: forward_step(2))
        pl.when(s == 3)(lambda: forward_step(3))

        @pl.when((s == 1) | (s == 2) | (s == 4))
        def _():
            differentiate(s - 1)

        @pl.when(s == 1)
        def _():
            hand_over(1)
            forward_step(1)

        pl.when(s == 2)(lambda: hand_over(2))
        pl.when(s == 4)(lambda: hand_over(6))
        pl.when(s < CHUNKS)(lambda: project(s))
        pl.when(s == 2)(lambda: hand_over(3))

        @pl.when(s == 3)
        def _():
            differentiate(2)
            hand_over(5)

        pl.when(s == 4)(lambda: hand_over(4, 7))

        @pl.when(s >= 3)
        def _():
            pair = jnp.where(s == 4, 2, jnp.where(s == 5, 1, s - 3))
            backproject(pair, s)

        @pl.when(s == 4)
        def _():
            differentiate(4)
            hand_over(8)

            @pl.when(jnp.logical_not(middle))
            def _():
                for n in range(2):
                    into_middle(2, n)

        @pl.when(s == 5)
        def _():
            for n in range(2):
                to_near(n)

        return carry

    lax.fori_loop(0, CHUNKS + 2, stage, 0)

    @pl.when(middle)
    def _():
        for n in range(PIECES):
            from_middle(3, n)

    @pl.when(jnp.logical_not(middle))
    def _():
        for n in (PIECES - 2, PIECES - 1):
            into_middle(3, n)

    def out_copy(n):
        return pltpu.make_async_copy(
            obuf.at[n], out_ref.at[:, pl.ds(pl.multiple_of(n * strip, 128), strip)], o_sem.at[n]
        )

    for k in range(4):
        gather_x(k).wait_send()
    for z in range(4):
        @at_place(z)
        def _(z=z):
            for copy in z_sends(z, (0, 1, 2)):
                copy.wait_send()
    for t in range(2):
        mate_sums(CHUNKS - 1, t).wait_send()

    def drain_sums(s, carry):
        each_half(s, lambda h: over_sums(s, h).wait_send())
        return carry

    def drain_grads(j, carry):
        over_grads(j, gy).wait_send()
        for n in range(2):
            mate_grads(j, gy, n).wait_send()
        return carry

    def drain_out(k, carry):
        for n in range(SENDS):
            out_x(k, n).wait_send()

        @pl.when((k == 1) | (k == 2))
        def _():
            for n in range(SENDS):
                to_owner(k, n, 0, near).wait_send()

        return carry

    lax.fori_loop(0, CHUNKS, drain_sums, 0)
    lax.fori_loop(1, 2 * CHUNKS - 1, drain_grads, 0)
    lax.fori_loop(0, 4, drain_out, 0)

    def finish(n, carry):
        out_x(0, n).wait_recv()
        total = wb[0, n] + xr[0, n].astype(F32)
        for lane in range(2):
            to_owner(1, n, lane, near).wait_recv()
            total = total + zr[lane, n].astype(F32)
        obuf[n] = total.astype(BF16)
        out_copy(n).start()
        return carry

    lax.fori_loop(0, SENDS, finish, 0)

    for n in range(SENDS):
        to_owner(3, n, 0, near).wait_send()
    for n in range(SENDS):
        out_copy(n).wait()


def fused(inputs, out_grad, gate_weight, up_weight, down_weight):
    rows, depth = inputs.shape
    width = gate_weight.shape[1]
    both, quarter, strip = 2 * rows, width // QUARTERS, depth // SENDS
    dma = pltpu.SemaphoreType.DMA
    n = CHUNKS
    scratch = [
        pltpu.VMEM((2, n * both, depth), BF16),
        pltpu.VMEM((depth, width), BF16),
        pltpu.VMEM((depth, width), BF16),
        pltpu.VMEM((width, depth), BF16),
        pltpu.VMEM((4, 3, both, quarter), F32),
        pltpu.VMEM((2, 2, 3, both, quarter), F32),
        pltpu.VMEM((2, 3, both, quarter), F32),
        pltpu.VMEM((n, 3, both, quarter), BF16),
        pltpu.VMEM((n, 3, both, quarter), BF16),
        pltpu.VMEM((2, n * both, width), BF16),
        pltpu.VMEM((4, SENDS, rows, strip), BF16),
        pltpu.VMEM((4, SENDS, rows, strip), BF16),
        pltpu.VMEM((4, SENDS, rows, strip), F32),
        pltpu.VMEM((4, SENDS, rows, strip), BF16),
        pltpu.VMEM((2, SENDS, rows, strip), BF16),
        pltpu.VMEM((2, SENDS, rows, strip), BF16),
        dma((2,)), dma((3, 4)), dma((2 * n,)), dma((4,)), dma((2, 4)), dma((2,)), dma((2, 2)),
        dma((n, 2)), dma((n, 2)), dma((2 * n,)), dma((2 * n,)), dma((2 * n, 2)), dma((2 * n, 2)),
        dma((4, SENDS)), dma((4, SENDS)), dma((4, SENDS)), dma((2, SENDS)), dma((2, SENDS)),
        pltpu.VMEM((SENDS, rows, strip), BF16), dma((SENDS,)),
    ]
    return pl.pallas_call(
        functools.partial(kernel, rows, depth, width),
        out_shape=jax.ShapeDtypeStruct((rows, depth), BF16),
        in_specs=[pl.BlockSpec(memory_space=pl.ANY)] * 5,
        out_specs=pl.BlockSpec(memory_space=pl.ANY),
        scratch_shapes=scratch,
        compiler_params=pltpu.CompilerParams(
            collective_id=0, has_side_effects=True, vmem_limit_bytes=66 * 1024 * 1000
        ),
    )(inputs, out_grad, gate_weight, up_weight, down_weight)


def plain(nx, ny, nz):
    def layer(inputs, out_grad, gate_weight, up_weight, down_weight):
        both = lax.all_gather(jnp.stack([inputs, out_grad]), ("gx", "gz"), axis=1, tiled=True)
        gate = jnp.dot(both[0], gate_weight, preferred_element_type=F32)
        upper = jnp.dot(both[0], up_weight, preferred_element_type=F32)
        hidden = contract_last(both[1], down_weight)
        terms = lax.psum_scatter(
            jnp.stack([gate, upper, hidden]), "gy", scatter_dimension=1, tiled=True
        )
        grads = jnp.stack(grads_of(terms[0], terms[1], terms[2]))
        grads = lax.all_gather(grads, "gy", axis=1, tiled=True)
        total = contract_last(grads[0], gate_weight) + contract_last(grads[1], up_weight)
        total = lax.psum_scatter(total, ("gx", "gz"), scatter_dimension=0, tiled=True)
        return total.astype(BF16)

    return layer


def solution(mesh):
    nx, ny, nz = mesh.shape["gx"], mesh.shape["gy"], mesh.shape["gz"]
    body = fused if (nx, ny, nz) == (2, 4, 4) else plain(nx, ny, nz)
    return jax.shard_map(body, mesh=mesh, in_specs=SPECS, out_specs=OUT_SPEC, check_vma=False)
```
